32 devices in a mesh: tp: 8 (over z, core), seq: 4 (over y, x).
Axes of the slice: x: 2, y: 2, z: 4, core: 2. Of those that a mesh axis runs over, the one named last changes fastest.
Arguments:
- residual: bfloat16 [1024, 4096], P('seq'), may hold values from -6 to 6
- mix_gain: float32 [4096], replicated, may hold values from 0.5 to 1.5
- in_proj: bfloat16 [4096, 4096], P(None, 'tp'), may hold values from -0.09375 to 0.09375
- branch_proj: bfloat16 [4096, 4096], P(None, 'tp'), may hold values from -0.09375 to 0.09375
- conv_weight: float32 [4, 4096], P(None, 'tp'), may hold values from -3 to 3
- conv_bias: float32 [4096], P('tp'), may hold values from -1.25 to 1.25
- input_gate: bfloat16 [16, 256, 256], P('tp'), may hold values from -0.375 to 0.375
- input_bias: float32 [4096], P('tp'), may hold values from -3 to 3
- decay_gate: bfloat16 [16, 256, 256], P('tp'), may hold values from -0.375 to 0.375
- decay_bias: float32 [4096], P('tp'), may hold values from -3 to 3
- decay_param: float32 [4096], P('tp'), may hold values from -13 to -2, as said below
- out_proj: bfloat16 [4096, 4096], P('tp'), may hold values from -0.25 to 0.25
- mlp_gain: float32 [4096], replicated, may hold values from 0.5 to 1.5
- gate_proj: bfloat16 [4096, 12288], P('seq', 'tp'), may hold values from -0.09375 to 0.09375
- up_proj: bfloat16 [4096, 12288], P('seq', 'tp'), may hold values from -0.09375 to 0.09375
- down_proj: bfloat16 [12288, 4096], P('tp'), may hold values from -0.078125 to 0.078125
Outputs:
- updated: bfloat16 [1024, 4096], P('seq')
The draws below stay inside these ranges and needn't reach their ends.
Inputs may be any that keep to these rules, and one draw needn't show every extreme that they name: softplus(decay_param) lies between 0.02 / 1024 and 0.1 for every channel.
All inputs are finite; a program needn't handle non-finite values.
Results may differ from the reference program's by a relative error of at most 0.02.
Values may be sent and summed in bfloat16 or wider, within the bound.
A program may use at most 128 MiB of HBM per device.

```python
import jax
import jax.numpy as jnp
from jax import lax

D = 4096
LRU = 4096
FF = 12288
HEADS = 16
CONV = 4
HEAD = 256
TOKENS = 1024


def draw_decay_param(key, part):
    lowest = 0.02 / TOKENS
    highest = 0.1
    spread = jax.random.uniform(key, (LRU,), jnp.float32)
    rate = lowest * jnp.exp(spread * jnp.log(highest / lowest))
    return jnp.log(jnp.expm1(rate)).astype(jnp.float32)


def raised(values, rng, source, target, shards_of, factor):
    owner, partner = [(jnp.arange(values.shape[axis_at]) // (values.shape[axis_at] // shards_of)).reshape([-1 if axis == axis_at else 1 for axis in range(values.ndim)]) for axis_at in (source, target)]
    chosen = jax.random.permutation(rng, shards_of)[partner]
    strong = (owner == chosen) | (owner == (partner + shards_of // 2) % shards_of)
    return jnp.where(strong, factor * values, values)


def steps_of(own_key, shape, shards, low, top_value):
    level = 1.0
    for axis_at, shards_of in shards:
        heights = jax.random.uniform(jax.random.fold_in(jax.random.fold_in(own_key, 6), axis_at), (shards_of,), jnp.float32, low / len(shards), top_value / len(shards))
        level = level * jnp.repeat(jnp.exp(heights), shape[axis_at] // shards_of).reshape((-1,) + (1,) * (len(shape) - 1 - axis_at))
    return level


def scatter_about(own_key, dims, deviation, bound, shards=(), dtype=jnp.bfloat16):
    values = jax.random.normal(own_key, dims, jnp.float32) * deviation
    if len(shards) > 0:
        values = steps_of(own_key, dims, shards, -0.22, 0.18) * values
    return jnp.clip(values, min=-bound, max=bound).astype(dtype)


def noise_with(own_key, extent, scale, most, cuts, heavy, dtype=jnp.bfloat16):
    drawn = scale * jax.random.normal(own_key, extent, jnp.float32)
    if cuts:
        drawn = drawn * steps_of(own_key, extent, cuts, -0.22, 0.18)
    return jnp.clip(raised(drawn, jax.random.fold_in(own_key, 3), *heavy), -most, most).astype(dtype)


def setup_inputs(seed: int = 0) -> dict:
    seeds = jax.random.split(jax.random.key(seed), 17)
    residual = scatter_about(seeds[0], (TOKENS, D), 1.0, 6.0, ((0, 4),))
    mix_gain = jnp.clip(1.0 + 0.1 * jax.random.normal(seeds[1], (D,), jnp.float32), 0.5, 1.5)
    in_proj = scatter_about(seeds[2], (D, LRU), D ** -0.5, 0.09375, ((1, 8),))
    branch_proj = scatter_about(seeds[3], (D, LRU), D ** -0.5, 0.09375, ((1, 8),))
    conv_weight = scatter_about(seeds[4], (CONV, LRU), CONV ** -0.5, 3.0, ((1, 8),), jnp.float32)
    conv_bias = scatter_about(seeds[5], (LRU,), 0.2, 1.25, ((0, 8),), jnp.float32)
    input_gate = scatter_about(seeds[6], (HEADS, HEAD, HEAD), HEAD ** -0.5, 0.375, ((0, 8),))
    input_bias = scatter_about(seeds[7], (LRU,), 0.5, 3.0, ((0, 8),), jnp.float32)
    decay_gate = scatter_about(seeds[8], (HEADS, HEAD, HEAD), HEAD ** -0.5, 0.375, ((0, 8),))
    decay_bias = scatter_about(seeds[9], (LRU,), 0.5, 3.0, ((0, 8),), jnp.float32)
    decay_param = draw_decay_param(jax.random.fold_in(seeds[16], 71), 0)
    out_proj = noise_with(seeds[11], (LRU, D), (LRU // 4) ** -0.5, 0.25, ((0, 8),), (0, 1, 8, 2.0))
    mlp_gain = jnp.clip(1.0 + 0.1 * jax.random.normal(seeds[12], (D,), jnp.float32), 0.5, 1.5)
    gate_proj = scatter_about(seeds[13], (D, FF), D ** -0.5, 0.09375, ((0, 4), (1, 8)))
    up_proj = scatter_about(seeds[14], (D, FF), D ** -0.5, 0.09375, ((0, 4), (1, 8)))
    down_proj = noise_with(seeds[15], (FF, D), FF ** -0.5, 0.078125, ((0, 8),), (0, 1, 8, 2.0))
    return {"residual": residual, "mix_gain": mix_gain, "in_proj": in_proj, "branch_proj": branch_proj, "conv_weight": conv_weight, "conv_bias": conv_bias, "input_gate": input_gate, "input_bias": input_bias, "decay_gate": decay_gate, "decay_bias": decay_bias, "decay_param": decay_param, "out_proj": out_proj, "mlp_gain": mlp_gain, "gate_proj": gate_proj, "up_proj": up_proj, "down_proj": down_proj}


epsilon = 1e-06

def rms_norm(values, gain):
    wide = values.astype(jnp.float32)
    factor = lax.rsqrt(lax.optimization_barrier(jnp.mean(wide * wide, axis=-1, keepdims=True)) + epsilon)
    return (wide * factor * gain).astype(jnp.bfloat16)

def block_gates(values, weight, bias):
    heads, width = (weight.shape[0], weight.shape[1])
    grouped = values.reshape(values.shape[0], heads, width).astype(jnp.float32)
    mixed = jnp.einsum('thi,hij->thj', grouped, weight.astype(jnp.float32))
    return jax.nn.sigmoid(mixed.reshape(values.shape[0], heads * width) + bias)

def smooth(inner, tail, conv_weight, conv_bias):
    taps = conv_weight.shape[0]
    length = inner.shape[0]
    padded = jnp.concatenate([tail, inner], axis=0).astype(jnp.float32)
    total = conv_bias + jnp.zeros((length, inner.shape[1]), jnp.float32)
    for offset in range(taps):
        total = total + conv_weight[offset] * padded[taps - 1 - offset:taps - 1 - offset + length]
    return lax.optimization_barrier(total.astype(jnp.bfloat16))

def advance(state, pair):
    state = pair[0] * state + pair[1]
    return (state, state)

def reference(residual, mix_gain, in_proj, branch_proj, conv_weight, conv_bias, input_gate, input_bias, decay_gate, decay_bias, decay_param, out_proj, mlp_gain, gate_proj, up_proj, down_proj):
    taps = conv_weight.shape[0]
    normed = rms_norm(residual, mix_gain)
    branch = jax.nn.gelu(jnp.dot(normed, branch_proj, preferred_element_type=jnp.float32), approximate=True)
    inner = jnp.dot(normed, in_proj, preferred_element_type=jnp.float32).astype(jnp.bfloat16)
    tail = jnp.zeros((taps - 1, inner.shape[1]), jnp.bfloat16)
    smoothed = smooth(inner, tail, conv_weight, conv_bias)
    input_rate = block_gates(smoothed, input_gate, input_bias)
    decay_rate = block_gates(smoothed, decay_gate, decay_bias)
    log_decay = -8.0 * decay_rate * jax.nn.softplus(decay_param)
    decay = jnp.exp(log_decay)
    first = (jnp.arange(TOKENS) == 0)[:, None]
    scale_in = jnp.where(first, 1.0, jnp.sqrt(-jnp.expm1(2.0 * log_decay)))
    pushed = smoothed.astype(jnp.float32) * input_rate * scale_in
    _, states = lax.scan(advance, jnp.zeros((LRU,), jnp.float32), (decay, pushed))
    gated = (states * branch).astype(jnp.bfloat16)
    mixed = jnp.dot(gated, out_proj, preferred_element_type=jnp.float32)
    middle = lax.optimization_barrier((residual.astype(jnp.float32) + mixed).astype(jnp.bfloat16))
    hidden_in = rms_norm(middle, mlp_gain)
    gate = jnp.dot(hidden_in, gate_proj, preferred_element_type=jnp.float32)
    up = jnp.dot(hidden_in, up_proj, preferred_element_type=jnp.float32)
    hidden = (jax.nn.gelu(gate, approximate=True) * up).astype(jnp.bfloat16)
    output = jnp.dot(hidden, down_proj, preferred_element_type=jnp.float32)
    return (middle.astype(jnp.float32) + output).astype(jnp.bfloat16)
```

```python
import functools

import jax
import jax.numpy as jnp
from jax import lax
from jax.experimental import pallas as pl
from jax.experimental.pallas import tpu as pltpu
from jax.sharding import PartitionSpec as P

epsilon = 1e-06
LOGICAL = pl.DeviceIdType.MESH
LANES = 128
EDGE = 16


def greet(axis, peers):
    barrier = pltpu.get_barrier_semaphore()
    for peer in peers:
        pl.semaphore_signal(barrier, inc=1, device_id={axis: peer}, device_id_type=LOGICAL)
    pl.semaphore_wait(barrier, len(peers))


def one_minus_exp(x):
    series = 1.0 + x * (1.0 / 9.0)
    for k in range(8, 1, -1):
        series = 1.0 + x * (1.0 / k) * series
    return jnp.where(x > -0.5, -x * series, 1.0 - jnp.exp(x))


def recurrence_kernel(
    count,
    taps,
    inner_ref,
    branch_ref,
    conv_weight_ref,
    conv_bias_ref,
    input_gate_ref,
    input_bias_ref,
    decay_gate_ref,
    decay_bias_ref,
    slope_ref,
    gated_ref,
    tail_ref,
    decays_ref,
    states_ref,
    ends_ref,
    arrived_ref,
    tail_send,
    tail_recv,
    end_send,
    end_recv,
):
    me = lax.axis_index("seq")
    length, channels = inner_ref.shape
    heads, head = input_gate_ref.shape[0], input_gate_ref.shape[1]
    peers = [lax.rem(me + offset, count) for offset in range(1, count)]
    greet("seq", peers)
    tail_copy = pltpu.make_async_remote_copy(
        src_ref=inner_ref.at[pl.ds(length - EDGE, EDGE), :],
        dst_ref=tail_ref,
        send_sem=tail_send,
        recv_sem=tail_recv,
        device_id={"seq": lax.rem(me + 1, count)},
        device_id_type=LOGICAL,
    )
    tail_copy.start()
    tail_copy.wait()
    follows = jnp.where(me > 0, 1.0, 0.0)

    for h in range(heads):
        columns = pl.ds(h * head, head)
        row = lax.broadcasted_iota(jnp.int32, (length, head), 0)
        current = inner_ref[:, columns].astype(jnp.float32)
        tail = tail_ref[:, columns].astype(jnp.float32) * follows
        before = jnp.concatenate([tail, jnp.zeros((length - EDGE, head), jnp.float32)], axis=0)
        total = conv_bias_ref[:, columns] + conv_weight_ref[0:1, columns] * current
        for tap in range(1, taps):
            shifted = jnp.where(
                row < tap,
                pltpu.roll(before, length + tap - EDGE, 0),
                pltpu.roll(current, tap, 0),
            )
            total = total + conv_weight_ref[tap : tap + 1, columns] * shifted
        smoothed = total.astype(jnp.bfloat16)
        input_rate = jax.nn.sigmoid(
            jnp.dot(smoothed, input_gate_ref[h], preferred_element_type=jnp.float32)
            + input_bias_ref[:, columns]
        )
        decay_rate = jax.nn.sigmoid(
            jnp.dot(smoothed, decay_gate_ref[h], preferred_element_type=jnp.float32)
            + decay_bias_ref[:, columns]
        )
        log_decay = decay_rate * slope_ref[:, columns]
        scale_in = jnp.sqrt(one_minus_exp(2.0 * log_decay))
        scale_in = jnp.where(jnp.logical_and(row == 0, me == 0), 1.0, scale_in)
        decays_ref[:, columns] = jnp.exp(log_decay)
        states_ref[:, columns] = smoothed.astype(jnp.float32) * input_rate * scale_in

    for c in range(channels // LANES):
        columns = pl.ds(c * LANES, LANES)
        row = lax.broadcasted_iota(jnp.int32, (length, LANES), 0)
        decay, state = decays_ref[:, columns], states_ref[:, columns]
        step = 1
        while step < length:
            reached = row >= step
            state = state + decay * jnp.where(reached, pltpu.roll(state, step, 0), 0.0)
            decay = decay * jnp.where(reached, pltpu.roll(decay, step, 0), 1.0)
            step *= 2
        decays_ref[:, columns] = decay
        states_ref[:, columns] = state
        ends_ref[0:1, columns] = decay[length - 1 :, :]
        ends_ref[1:2, columns] = state[length - 1 :, :]

    copies = [
        pltpu.make_async_remote_copy(
            src_ref=ends_ref,
            dst_ref=arrived_ref.at[k],
            send_sem=end_send.at[k],
            recv_sem=end_recv.at[k],
            device_id={"seq": peers[k]},
            device_id_type=LOGICAL,
        )
        for k in range(count - 1)
    ]
    for copy in copies:
        copy.start()
    for copy in copies:
        copy.wait()
    carried = jnp.zeros((1, channels), jnp.float32)
    for k in range(count - 2, -1, -1):
        new = arrived_ref[k, 0:1, :] * carried + arrived_ref[k, 1:2, :]
        carried = jnp.where(me >= k + 1, new, carried)
    gated_ref[...] = (
        (states_ref[...] + decays_ref[...] * carried) * branch_ref[...]
    ).astype(jnp.bfloat16)


def recurrence(inner, branch, conv_weight, conv_bias, input_gate, input_bias, decay_gate, decay_bias, slope):
    count = lax.axis_size("seq")
    length, channels = inner.shape
    vmem = pl.BlockSpec(memory_space=pltpu.VMEM)
    return pl.pallas_call(
        functools.partial(recurrence_kernel, count, conv_weight.shape[0]),
        out_shape=jax.ShapeDtypeStruct((length, channels), jnp.bfloat16),
        in_specs=[vmem] * 9,
        out_specs=vmem,
        scratch_shapes=[
            pltpu.VMEM((EDGE, channels), jnp.bfloat16),
            pltpu.VMEM((length, channels), jnp.float32),
            pltpu.VMEM((length, channels), jnp.float32),
            pltpu.VMEM((8, channels), jnp.float32),
            pltpu.VMEM((count - 1, 8, channels), jnp.float32),
            pltpu.SemaphoreType.DMA,
            pltpu.SemaphoreType.DMA,
            pltpu.SemaphoreType.DMA((count - 1,)),
            pltpu.SemaphoreType.DMA((count - 1,)),
        ],
        compiler_params=pltpu.CompilerParams(
            collective_id=0, has_side_effects=True, vmem_limit_bytes=24 * 2**20
        ),
    )(
        inner,
        branch,
        conv_weight,
        conv_bias[None],
        input_gate,
        input_bias[None],
        decay_gate,
        decay_bias[None],
        slope[None],
    )


def summed_rows(product, extent, axis):
    everything = product(jnp.int32(0), lax.axis_size(axis) * extent)
    own = lax.psum_scatter(everything.astype(jnp.bfloat16), axis, scatter_dimension=0, tiled=True)
    return own.astype(jnp.float32)


def rms_norm(values, gain):
    wide = values.astype(jnp.float32)
    factor = lax.rsqrt(jnp.mean(wide * wide, axis=-1, keepdims=True) + epsilon)
    return (wide * factor * gain).astype(jnp.bfloat16)


def channel_total(partial_value):
    return lax.psum(partial_value.astype(jnp.bfloat16), "tp").astype(jnp.float32)


def on_device(
    residual,
    mix_gain,
    in_proj,
    branch_proj,
    conv_weight,
    conv_bias,
    input_gate,
    input_bias,
    decay_gate,
    decay_bias,
    decay_param,
    out_proj,
    mlp_gain,
    gate_proj,
    up_proj,
    down_proj,
):
    length = residual.shape[0]
    normed = rms_norm(residual, mix_gain)
    branch = jax.nn.gelu(
        jnp.dot(normed, branch_proj, preferred_element_type=jnp.float32), approximate=True
    )
    inner = jnp.dot(normed, in_proj, preferred_element_type=jnp.float32).astype(jnp.bfloat16)
    gated = recurrence(
        inner,
        branch,
        conv_weight,
        conv_bias,
        input_gate,
        input_bias,
        decay_gate,
        decay_bias,
        -8.0 * jax.nn.softplus(decay_param),
    )
    mixed = channel_total(jnp.dot(gated, out_proj, preferred_element_type=jnp.float32))
    middle = lax.optimization_barrier((residual.astype(jnp.float32) + mixed).astype(jnp.bfloat16))
    hidden_in = rms_norm(middle, mlp_gain)
    width = gate_proj.shape[1]
    columns = lax.all_to_all(hidden_in, "seq", split_axis=1, concat_axis=0, tiled=True)

    def term(start, count):
        block = lax.dynamic_slice_in_dim(columns, start, count, 0)
        return jnp.concatenate(
            [
                jnp.dot(block, gate_proj, preferred_element_type=jnp.float32),
                jnp.dot(block, up_proj, preferred_element_type=jnp.float32),
            ],
            axis=1,
        )

    joined = summed_rows(term, length, "seq")
    gate = joined[:, :width]
    up = joined[:, width:]
    hidden = (jax.nn.gelu(gate, approximate=True) * up).astype(jnp.bfloat16)
    output = channel_total(jnp.dot(hidden, down_proj, preferred_element_type=jnp.float32))
    return (middle.astype(jnp.float32) + output).astype(jnp.bfloat16)


def solution(mesh):
    in_specs = (
        P("seq", None),
        P(),
        P(None, "tp"),
        P(None, "tp"),
        P(None, "tp"),
        P("tp"),
        P("tp", None, None),
        P("tp"),
        P("tp", None, None),
        P("tp"),
        P("tp"),
        P("tp", None),
        P(),
        P("seq", "tp"),
        P("seq", "tp"),
        P("tp", None),
    )
    out_specs = P("seq", None)
    return jax.shard_map(
        on_device, mesh=mesh, in_specs=in_specs, out_specs=out_specs, check_vma=False
    )
```

```python
import functools

import jax
import jax.numpy as jnp
from jax import lax
from jax.experimental import pallas as pl
from jax.experimental.pallas import tpu as pltpu
from jax.sharding import PartitionSpec as P

epsilon = 1e-06
LOGICAL = pl.DeviceIdType.MESH
LANES = 128
EDGE = 16
HEIGHT = 16
LAG = 4


def greet(axis, peers):
    barrier = pltpu.get_barrier_semaphore()
    for peer in peers:
        pl.semaphore_signal(barrier, inc=1, device_id={axis: peer}, device_id_type=LOGICAL)
    pl.semaphore_wait(barrier, len(peers))


def one_minus_exp(x):
    series = 1.0 + x * (1.0 / 9.0)
    for k in range(8, 1, -1):
        series = 1.0 + x * (1.0 / k) * series
    return jnp.where(x > -0.5, -x * series, 1.0 - jnp.exp(x))


def recurrence_kernel(
    count,
    taps,
    inner_ref,
    branch_ref,
    conv_weight_ref,
    conv_bias_ref,
    input_gate_ref,
    input_bias_ref,
    decay_gate_ref,
    decay_bias_ref,
    slope_ref,
    gated_ref,
    tail_ref,
    decays_ref,
    states_ref,
    ends_ref,
    arrived_ref,
    tail_send,
    tail_recv,
    end_send,
    end_recv,
):
    me = lax.axis_index("seq")
    length, channels = inner_ref.shape
    heads, head = input_gate_ref.shape[0], input_gate_ref.shape[1]
    peers = [lax.rem(me + offset, count) for offset in range(1, count)]
    greet("seq", peers)
    tail_copy = pltpu.make_async_remote_copy(
        src_ref=inner_ref.at[pl.ds(length - EDGE, EDGE), :],
        dst_ref=tail_ref,
        send_sem=tail_send,
        recv_sem=tail_recv,
        device_id={"seq": lax.rem(me + 1, count)},
        device_id_type=LOGICAL,
    )
    tail_copy.start()
    tail_copy.wait()
    follows = jnp.where(me > 0, 1.0, 0.0)

    for h in range(heads):
        columns = pl.ds(h * head, head)
        row = lax.broadcasted_iota(jnp.int32, (length, head), 0)
        current = inner_ref[:, columns].astype(jnp.float32)
        tail = tail_ref[:, columns].astype(jnp.float32) * follows
        before = jnp.concatenate([tail, jnp.zeros((length - EDGE, head), jnp.float32)], axis=0)
        total = conv_bias_ref[:, columns] + conv_weight_ref[0:1, columns] * current
        for tap in range(1, taps):
            shifted = jnp.where(
                row < tap,
                pltpu.roll(before, length + tap - EDGE, 0),
                pltpu.roll(current, tap, 0),
            )
            total = total + conv_weight_ref[tap : tap + 1, columns] * shifted
        smoothed = total.astype(jnp.bfloat16)
        input_rate = jax.nn.sigmoid(
            jnp.dot(smoothed, input_gate_ref[h], preferred_element_type=jnp.float32)
            + input_bias_ref[:, columns]
        )
        decay_rate = jax.nn.sigmoid(
            jnp.dot(smoothed, decay_gate_ref[h], preferred_element_type=jnp.float32)
            + decay_bias_ref[:, columns]
        )
        log_decay = decay_rate * slope_ref[:, columns]
        scale_in = jnp.sqrt(one_minus_exp(2.0 * log_decay))
        scale_in = jnp.where(jnp.logical_and(row == 0, me == 0), 1.0, scale_in)
        decays_ref[:, columns] = jnp.exp(log_decay)
        states_ref[:, columns] = smoothed.astype(jnp.float32) * input_rate * scale_in

    for c in range(channels // LANES):
        columns = pl.ds(c * LANES, LANES)
        row = lax.broadcasted_iota(jnp.int32, (length, LANES), 0)
        decay, state = decays_ref[:, columns], states_ref[:, columns]
        step = 1
        while step < length:
            reached = row >= step
            state = state + decay * jnp.where(reached, pltpu.roll(state, step, 0), 0.0)
            decay = decay * jnp.where(reached, pltpu.roll(decay, step, 0), 1.0)
            step *= 2
        decays_ref[:, columns] = decay
        states_ref[:, columns] = state
        ends_ref[0:1, columns] = decay[length - 1 :, :]
        ends_ref[1:2, columns] = state[length - 1 :, :]

    copies = [
        pltpu.make_async_remote_copy(
            src_ref=ends_ref,
            dst_ref=arrived_ref.at[k],
            send_sem=end_send.at[k],
            recv_sem=end_recv.at[k],
            device_id={"seq": peers[k]},
            device_id_type=LOGICAL,
        )
        for k in range(count - 1)
    ]
    for copy in copies:
        copy.start()
    for copy in copies:
        copy.wait()
    carried = jnp.zeros((1, channels), jnp.float32)
    for k in range(count - 2, -1, -1):
        new = arrived_ref[k, 0:1, :] * carried + arrived_ref[k, 1:2, :]
        carried = jnp.where(me >= k + 1, new, carried)
    gated_ref[...] = (
        (states_ref[...] + decays_ref[...] * carried) * branch_ref[...]
    ).astype(jnp.bfloat16)


def recurrence(inner, branch, conv_weight, conv_bias, input_gate, input_bias, decay_gate, decay_bias, slope):
    count = lax.axis_size("seq")
    length, channels = inner.shape
    vmem = pl.BlockSpec(memory_space=pltpu.VMEM)
    return pl.pallas_call(
        functools.partial(recurrence_kernel, count, conv_weight.shape[0]),
        out_shape=jax.ShapeDtypeStruct((length, channels), jnp.bfloat16),
        in_specs=[vmem] * 9,
        out_specs=vmem,
        scratch_shapes=[
            pltpu.VMEM((EDGE, channels), jnp.bfloat16),
            pltpu.VMEM((length, channels), jnp.float32),
            pltpu.VMEM((length, channels), jnp.float32),
            pltpu.VMEM((8, channels), jnp.float32),
            pltpu.VMEM((count - 1, 8, channels), jnp.float32),
            pltpu.SemaphoreType.DMA,
            pltpu.SemaphoreType.DMA,
            pltpu.SemaphoreType.DMA((count - 1,)),
            pltpu.SemaphoreType.DMA((count - 1,)),
        ],
        compiler_params=pltpu.CompilerParams(
            collective_id=0, has_side_effects=True, vmem_limit_bytes=24 * 2**20
        ),
    )(
        inner,
        branch,
        conv_weight,
        conv_bias[None],
        input_gate,
        input_bias[None],
        decay_gate,
        decay_bias[None],
        slope[None],
    )


def summed_rows(product, extent, axis):
    everything = product(jnp.int32(0), lax.axis_size(axis) * extent)
    own = lax.psum_scatter(everything.astype(jnp.bfloat16), axis, scatter_dimension=0, tiled=True)
    return own.astype(jnp.float32)


def rms_norm(values, gain):
    wide = values.astype(jnp.float32)
    factor = lax.rsqrt(jnp.mean(wide * wide, axis=-1, keepdims=True) + epsilon)
    return (wide * factor * gain).astype(jnp.bfloat16)


def summed_kernel(
    chips,
    part_ref,
    base_ref,
    out_ref,
    pair_ref,
    stage_ref,
    left_ref,
    right_ref,
    pair_send,
    pair_recv,
    line_send,
    left_recv,
    right_recv,
    out_send,
    out_recv,
    share_send,
    share_recv,
):
    me = lax.axis_index("tp")
    core, chip = lax.rem(me, 2), lax.div(me, 2)
    partner = me + 1 - 2 * core
    pieces, height = stage_ref.shape[0], stage_ref.shape[1]
    half = pieces * height
    ring = [partner, lax.rem(me + 2, 2 * chips), lax.rem(me + 2 * chips - 2, 2 * chips)]
    greet("tp", ring)

    def rows(which, p):
        return pl.ds(pl.multiple_of(which * half + p * height, height), height)

    def remote(source, target, send, recv, device):
        return pltpu.make_async_remote_copy(
            src_ref=source,
            dst_ref=target,
            send_sem=send,
            recv_sem=recv,
            device_id={"tp": device},
            device_id_type=LOGICAL,
        )

    def pair(p):
        return remote(
            part_ref.at[rows(1 - core, p), :], pair_ref.at[p], pair_send.at[p], pair_recv.at[p], partner
        )

    def rightward(p):
        return remote(stage_ref.at[p], left_ref.at[p], line_send.at[p], left_recv.at[p], me + 2)

    def leftward(p):
        return remote(stage_ref.at[p], right_ref.at[p], line_send.at[p], right_recv.at[p], me - 2)

    def outward(p, way):
        mine = out_ref.at[rows(core, p), :]
        return remote(mine, mine, out_send.at[way, p], out_recv.at[p], me + 4 * way - 2)

    def share(p, which):
        block = out_ref.at[rows(which, p), :]
        return remote(block, block, share_send.at[p], share_recv.at[p], partner)

    for p in range(pieces):
        pair(p).start()

    def run(z):
        sent = []

        def owner(p):
            return chips // 2 - p % 2

        def start(copy):
            copy.start()
            sent.append(copy)

        def reduce(p):
            pair(p).wait_recv()
            value = part_ref[rows(core, p), :].astype(jnp.float32) + pair_ref[p].astype(jnp.float32)
            if z > 0 and z <= owner(p):
                rightward(p).wait_recv()
                value = value + left_ref[p].astype(jnp.float32)
            if z < chips - 1 and z >= owner(p):
                leftward(p).wait_recv()
                value = value + right_ref[p].astype(jnp.float32)
            if z == owner(p):
                total = value + base_ref[rows(core, p), :].astype(jnp.float32)
                out_ref[rows(core, p), :] = total.astype(out_ref.dtype)
                if z > 0:
                    start(outward(p, 0))
                if z < chips - 1:
                    start(outward(p, 1))
                start(share(p, core))
            else:
                stage_ref[p] = value.astype(stage_ref.dtype)
                start(rightward(p) if z < owner(p) else leftward(p))

        def spread(p):
            if z == owner(p):
                return
            outward(p, 0).wait_recv()
            if z < owner(p) and z > 0:
                start(outward(p, 0))
            if z > owner(p) and z < chips - 1:
                start(outward(p, 1))
            start(share(p, core))

        lag = pieces if z in (0, chips - 1) else min(pieces, LAG)
        for p in range(pieces + lag):
            if p < pieces:
                reduce(p)
            if p >= lag:
                spread(p - lag)
        for copy in sent:
            copy.wait_send()

    for z in range(chips):
        pl.when(chip == z)(functools.partial(run, z))
    for p in range(pieces):
        pair(p).wait_send()
        share(p, 1 - core).wait_recv()


def summed(part, base, call):
    chips = lax.axis_size("tp") // 2
    length, width = part.shape
    pieces = length // (2 * HEIGHT)
    vmem = pl.BlockSpec(memory_space=pltpu.VMEM)
    block = pltpu.VMEM((pieces, HEIGHT, width), jnp.bfloat16)
    semaphores = pltpu.SemaphoreType.DMA((pieces,))
    return pl.pallas_call(
        functools.partial(summed_kernel, chips),
        out_shape=jax.ShapeDtypeStruct((length, width), jnp.bfloat16),
        in_specs=[vmem] * 2,
        out_specs=vmem,
        scratch_shapes=[block] * 4
        + [semaphores] * 5
        + [pltpu.SemaphoreType.DMA((2, pieces))]
        + [semaphores] * 3,
        compiler_params=pltpu.CompilerParams(
            collective_id=call, has_side_effects=True, vmem_limit_bytes=24 * 2**20
        ),
    )(part, base)


def on_device(
    residual,
    mix_gain,
    in_proj,
    branch_proj,
    conv_weight,
    conv_bias,
    input_gate,
    input_bias,
    decay_gate,
    decay_bias,
    decay_param,
    out_proj,
    mlp_gain,
    gate_proj,
    up_proj,
    down_proj,
):
    length = residual.shape[0]
    normed = rms_norm(residual, mix_gain)
    branch = jax.nn.gelu(
        jnp.dot(normed, branch_proj, preferred_element_type=jnp.float32), approximate=True
    )
    inner = jnp.dot(normed, in_proj, preferred_element_type=jnp.float32).astype(jnp.bfloat16)
    gated = recurrence(
        inner,
        branch,
        conv_weight,
        conv_bias,
        input_gate,
        input_bias,
        decay_gate,
        decay_bias,
        -8.0 * jax.nn.softplus(decay_param),
    )
    mixed = jnp.dot(gated, out_proj, preferred_element_type=jnp.float32).astype(jnp.bfloat16)
    middle = summed(mixed, residual, 1)
    hidden_in = rms_norm(middle, mlp_gain)
    width = gate_proj.shape[1]
    columns = lax.all_to_all(hidden_in, "seq", split_axis=1, concat_axis=0, tiled=True)

    def term(start, count):
        block = lax.dynamic_slice_in_dim(columns, start, count, 0)
        return jnp.concatenate(
            [
                jnp.dot(block, gate_proj, preferred_element_type=jnp.float32),
                jnp.dot(block, up_proj, preferred_element_type=jnp.float32),
            ],
            axis=1,
        )

    joined = summed_rows(term, length, "seq")
    gate = joined[:, :width]
    up = joined[:, width:]
    hidden = (jax.nn.gelu(gate, approximate=True) * up).astype(jnp.bfloat16)
    output = jnp.dot(hidden, down_proj, preferred_element_type=jnp.float32).astype(jnp.bfloat16)
    return summed(output, middle, 2)


def solution(mesh):
    in_specs = (
        P("seq", None),
        P(),
        P(None, "tp"),
        P(None, "tp"),
        P(None, "tp"),
        P("tp"),
        P("tp", None, None),
        P("tp"),
        P("tp", None, None),
        P("tp"),
        P("tp"),
        P("tp", None),
        P(),
        P("seq", "tp"),
        P("seq", "tp"),
        P("tp", None),
    )
    out_specs = P("seq", None)
    return jax.shard_map(
        on_device, mesh=mesh, in_specs=in_specs, out_specs=out_specs, check_vma=False
    )
```
